32 devices in a mesh: gx: 2 (over y), gy: 4 (over z), gz: 4 (over x, core).
Axes of the slice: x: 2, y: 2, z: 4, core: 2. Of those that a mesh axis runs over, the one named last changes fastest.
Arguments:
- blocks: bfloat16 [1600, 64, 4096], P(('gx', 'gy', 'gz')), may hold values from -6 to 6
- ownership: int32 [1600, 3], P(('gx', 'gy', 'gz')), may hold values from -1 to 15, as said below
- basis_rows: bfloat16 [1024, 48], replicated, may hold values from -0.1875 to 0.1875
Outputs:
- gram_matrix: float32 [1024, 1024], P(('gx', 'gy', 'gz'))
The draws below stay inside these ranges and needn't reach their ends.
Inputs may be any that keep to these rules, and one draw needn't show every extreme that they name: `ownership`: row d * 50 + s is slot s of device d in mesh order. Each row is a block triple (i, j, k) with i <= j <= k, or -1 -1 -1 for an empty slot; every such triple of blocks 0 to 15 stands in exactly one row; the live slots of a device come first; some device has all 50 slots live.
All inputs are finite; a program needn't handle non-finite values.
Results may differ from the reference program's by a relative error of at most 0.0037.
Values may be sent and summed in bfloat16 or wider, within the bound.
A program may use at most 192 MiB of HBM per device.

```python
import jax
import jax.numpy as jnp
import numpy as np
from jax import lax

N = 1024
NB = 16
R = 48
BS = 64
NUNIQ = 816
SLOTS = 50
DEVICES = 32


def draw_ownership(key, part):
    listing = np.array([[lead_block, mid_block, tail_block] for lead_block in range(NB) for mid_block in range(lead_block, NB) for tail_block in range(mid_block, NB)], dtype=np.int32)
    shuffled = jnp.asarray(listing)[jax.random.permutation(jax.random.fold_in(key, 11), listing.shape[0])]
    ranking = jax.random.permutation(jax.random.fold_in(key, 12), DEVICES)
    base_load = NUNIQ // DEVICES
    extra_load = NUNIQ % DEVICES
    loads = base_load + (ranking < extra_load).astype(jnp.int32) + jnp.where(ranking % 2 == 0, base_load - 1, 1 - base_load)
    offsets = jnp.cumsum(loads) - loads
    slot_ids = jnp.arange(SLOTS, dtype=jnp.int32)
    wanted = offsets[:, None] + slot_ids[None, :]
    live = slot_ids[None, :] < loads[:, None]
    selected_rows = shuffled[jnp.clip(wanted, 0, NUNIQ - 1)]
    return jnp.where(live[:, :, None], selected_rows, -1).reshape(DEVICES * SLOTS, 3).astype(jnp.int32)


def block_levels(stream_key, shape, pieces, smallest, largest):
    level = 1.0
    for dim, blocks in pieces:
        draws = jax.random.uniform(jax.random.fold_in(jax.random.fold_in(stream_key, 6), dim), (blocks,), jnp.float32, smallest / len(pieces), largest / len(pieces))
        level = level * jnp.repeat(jnp.exp(draws), shape[dim] // blocks).reshape((-1,) + (1,) * (len(shape) - 1 - dim))
    return level


def scatter_about(stream_key, dims, deviation, most, pieces=(), kind=jnp.bfloat16):
    values = deviation * jax.random.normal(stream_key, dims, jnp.float32)
    if pieces:
        values = values * block_levels(stream_key, dims, pieces, -0.22, 0.18)
    return jnp.clip(values, -most, most).astype(kind)


def setup_inputs(seed: int = 0) -> dict:
    arg_keys = jax.random.split(jax.random.key(seed), 4)
    blocks = scatter_about(arg_keys[0], (DEVICES * SLOTS, BS, BS * BS), 1.0, 6.0, ((0, 32),))
    ownership = draw_ownership(jax.random.fold_in(arg_keys[3], 71), 0)
    basis_rows = scatter_about(arg_keys[2], (N, R), N ** -0.5, 0.1875)
    return dict(blocks=blocks, ownership=ownership, basis_rows=basis_rows)


ORDERS = ((0, 1, 2), (0, 2, 1), (1, 0, 2), (1, 2, 0), (2, 0, 1), (2, 1, 0))
REDUCE_FORMS = ("gxyz,gxq->gyzq", "gxyz,gyq->gxzq", "gxyz,gzq->gxyq")


def unpack(stored, unique_triples):
    number = stored.shape[0]
    extent = stored.shape[1]
    unpacked = stored.reshape(number, extent, extent, extent)
    leading_block_index = lax.broadcasted_iota(jnp.int32, (1, extent, extent, extent), 1)
    middle = lax.broadcasted_iota(jnp.int32, (1, extent, extent, extent), 2)
    trailing = lax.broadcasted_iota(jnp.int32, (1, extent, extent, extent), 3)
    same_front = (unique_triples[:, 0] == unique_triples[:, 1])[:, None, None, None]
    same_back = (unique_triples[:, 1] == unique_triples[:, 2])[:, None, None, None]

    def order_back(values):
        return jnp.where(middle <= trailing, values, jnp.swapaxes(values, 2, 3))

    def order_front(values):
        return jnp.where(leading_block_index <= middle, values, jnp.swapaxes(values, 1, 2))

    unpacked = jnp.where(same_back, order_back(unpacked), unpacked)
    unpacked = jnp.where(same_front, order_front(unpacked), unpacked)
    unpacked = jnp.where(same_back, order_back(unpacked), unpacked)
    return unpacked


def slot_terms(stored, unique_triples, basis_rows):
    extent = stored.shape[1]
    columns = basis_rows.shape[1]
    unpacked = unpack(stored, unique_triples).astype(jnp.float32)
    basis_blocks = basis_rows.reshape(basis_rows.shape[0] // extent, extent, columns)
    selected_rows = jnp.take(basis_blocks, jnp.clip(unique_triples, 0, basis_blocks.shape[0] - 1), axis=0).astype(jnp.float32)
    factors = (selected_rows[:, 0], selected_rows[:, 1], selected_rows[:, 2])
    reduced = [jnp.einsum(REDUCE_FORMS[slot_pos], unpacked, factors[slot_pos]).astype(jnp.bfloat16).astype(jnp.float32) for slot_pos in range(3)]
    by_row = [0.0, 0.0, 0.0]
    for position in range(6):
        row_slot_index, middle_slot_index, last_slot = ORDERS[position]
        contraction_form = "zixl,zxo->ziol" if row_slot_index < middle_slot_index else "hwie,hwy->hiye"
        contrib = jnp.einsum(contraction_form, reduced[last_slot], factors[middle_slot_index])
        ordered = unique_triples[:, jnp.array(ORDERS[position])]
        distinct = unique_triples[:, 0] >= 0
        for earlier in ORDERS[:position]:
            distinct = distinct & jnp.any(ordered != unique_triples[:, jnp.array(earlier)], axis=1)
        by_row[row_slot_index] = by_row[row_slot_index] + jnp.where(distinct[:, None, None, None], contrib, 0.0)
    stacked = jnp.stack(by_row, axis=1)
    return stacked.reshape(stacked.shape[0], 3, extent, columns * columns)


def reference(blocks, ownership, basis_rows):
    extent = N // NB
    per_turn = 16
    turns = blocks.shape[0] // per_turn
    stored_all = blocks.reshape(turns, per_turn, extent, extent * extent)
    owned_all = ownership.reshape(turns, per_turn, 3)

    def scan_step(accumulated, scan_item):
        stored, unique_triples = scan_item
        contribs = slot_terms(stored, unique_triples, basis_rows)
        targets = jnp.clip(unique_triples, 0, NB - 1).reshape(-1).astype(jnp.int32)
        accumulated = accumulated.at[targets].add(contribs.reshape(-1, extent, R * R))
        return accumulated, None

    zero_rows = jnp.zeros((NB, extent, R * R), jnp.float32)
    summed, _ = lax.scan(scan_step, zero_rows, (stored_all, owned_all))
    product = summed.reshape(N, R, R)
    symmetric = (0.5 * (product + jnp.swapaxes(product, 1, 2))).reshape(N, R * R)
    rounded = symmetric.astype(jnp.bfloat16)
    return jnp.dot(rounded, rounded.T, preferred_element_type=jnp.float32) / R
```

```python
import functools

import jax
import jax.numpy as jnp
from jax import lax
from jax.experimental import pallas as pl
from jax.experimental.pallas import tpu as pltpu
from jax.sharding import PartitionSpec as P

AXES = ("gx", "gy", "gz")
DEPTH = 3
f32, bf16 = jnp.float32, jnp.bfloat16
MESH = pl.DeviceIdType.MESH


def contract_kernel(nb, ext, rank, own, count, blocks, ut, utp, ub, out, accv, accw, buf, sems, bd, mask, sv, sw, vb, pk, turning):
    half = ext // 2
    pitch = half + 1
    width = 4 * ext
    chunks = ext * ext // width
    low_rank = rank // 2
    n = count[0]

    def fetch(s):
        return pltpu.make_async_copy(blocks.at[s], buf.at[lax.rem(s, DEPTH)], sems.at[lax.rem(s, DEPTH)])

    for s in range(DEPTH - 1):
        @pl.when(s < n)
        def _():
            fetch(s).start()

    lane = lax.broadcasted_iota(jnp.int32, (ext, width), 1)
    row = lax.broadcasted_iota(jnp.int32, (ext, width), 0)

    def prepare(b, _):
        u = ub[b]
        u4 = jnp.concatenate([u, u, u, u], axis=1)
        for y in range(4):
            bd[b, y * ext:(y + 1) * ext, :] = jnp.where(lane // ext == y, u4, 0)
        accv[b] = jnp.zeros(accv.shape[1:], f32)
        accw[b] = jnp.zeros(accw.shape[1:], f32)
        return 0

    lax.fori_loop(0, nb, prepare, 0)

    for c in range(chunks):
        y = lane // ext + 4 * c
        z = lax.rem(lane, ext)
        front = jnp.where(row < y, 1.0, jnp.where(row == y, 0.5, 0.0))
        back = jnp.where(y < z, 1.0, jnp.where(y == z, 0.5, 0.0))
        both = jnp.where((row == y) & (y == z), 1.0 / 6.0, front * back)
        cols = slice(c * width, (c + 1) * width)
        mask[0, :, cols] = front.astype(bf16)
        mask[1, :, cols] = back.astype(bf16)
        mask[2, :, cols] = both.astype(bf16)

    def halves(a, b):
        low = lax.broadcasted_iota(jnp.int32, a.shape, 1) < ext
        return jnp.where(low, a, pltpu.roll(b, ext, 1)), jnp.where(low, pltpu.roll(a, ext, 1), b)

    def gather(src, first):
        e0, e1 = halves(src[pl.ds(first * pitch, half), :], src[pl.ds((first + 1) * pitch, half), :])
        return jnp.concatenate([e0, e1], axis=0).astype(bf16)

    def step(s, _):
        cur = lax.rem(s, DEPTH)
        fetch(s).wait()

        @pl.when(s + DEPTH - 1 < n)
        def _():
            fetch(s + DEPTH - 1).start()

        i, j, k = own[3 * s], own[3 * s + 1], own[3 * s + 2]
        kind = jnp.where(j == k, jnp.where(i == j, 2, 1), 0)

        @pl.when((i == j) | (j == k))
        def _():
            for c in range(chunks):
                cols = slice(c * width, (c + 1) * width)
                buf[cur, :, cols] = buf[cur, :, cols] * mask[kind, :, cols]

        ui = ut[i]
        uj = utp[j]
        bdk = bd[k]
        for c in range(chunks):
            cols = slice(c * width, (c + 1) * width)
            t = buf[cur, :, cols]
            v = jnp.dot(t, bdk, preferred_element_type=f32)
            sv[pl.ds(2 * c, ext, stride=pitch), :] = v[:, :128]
            sv[pl.ds(2 * c + 1, ext, stride=pitch), :] = v[:, 128:]
            vb[:, cols] = v.astype(bf16)
            w = jnp.dot(ui, t, preferred_element_type=f32)
            sw[pl.ds(2 * c, rank, stride=pitch), :] = w[:, :128]
            sw[pl.ds(2 * c + 1, rank, stride=pitch), :] = w[:, 128:]
        for c in range(chunks):
            cols = slice(c * width, (c + 1) * width)
            accv[j, :, cols] += jnp.dot(ui, vb[:, cols], preferred_element_type=f32)
        for c in range(chunks):
            cols = slice(c * width, (c + 1) * width)
            e = jnp.concatenate([gather(sv, 4 * c), gather(sv, 4 * c + 2)], axis=1)
            accv[i, :, cols] += jnp.dot(uj, e, preferred_element_type=f32)
        for c in range(rank * ext // width):
            cols = slice(c * width, (c + 1) * width)
            e = jnp.concatenate([gather(sw, 4 * c), gather(sw, 4 * c + 2)], axis=1)
            accw[k, :, cols] += jnp.dot(uj, e, preferred_element_type=f32)
        return 0

    lax.fori_loop(0, n, step, 0)

    def spread(x, b):
        l = lax.rem(lax.broadcasted_iota(jnp.int32, x.shape, 1), ext)
        if b < 2:
            return pltpu.roll(x, low_rank - 8 * b, 1)
        return jnp.where(l < rank + 8, pltpu.roll(x, low_rank - 8 * b, 1), pltpu.roll(x, low_rank + 8, 1))

    def stack(a, b):
        pad = jnp.zeros((ext - rank, 128), f32)
        return jnp.concatenate([a, pad, b, pad], axis=0)

    def finish(t, _):
        for g in range(half // 2):
            p0, p1 = accv[t, :, 256 * g:256 * g + 128], accv[t, :, 256 * g + 128:256 * g + 256]
            turning[g] = stack(*halves(p0, p1))
        for g in range(half // 2):
            turned = jnp.transpose(turning[g])
            for h in range(2):
                cols = slice((2 * g + h) * 128, (2 * g + h + 1) * 128)
                accv[t, :, cols] += turned[h * ext:h * ext + rank]
        for g in range(half):
            s = accv[t, :, g * 128:(g + 1) * 128]
            l = lax.rem(lax.broadcasted_iota(jnp.int32, (8, 128), 1), ext)
            for b in range(3):
                piece = jnp.where(l < rank, s[8 * b:8 * b + 8], spread(s[low_rank + 8 * b:low_rank + 8 * b + 8], b))
                sv[pl.ds(8 * b * pitch + g, 8, stride=pitch), :] = piece
        wpitch = low_rank + 1
        for c in range(low_rank):
            sw[pl.ds(c, rank, stride=wpitch), :] = accw[t, :, c * 128:(c + 1) * 128]
        for c in range(low_rank):
            e0, e1 = halves(sw[pl.ds(2 * c * wpitch, low_rank), :], sw[pl.ds((2 * c + 1) * wpitch, low_rank), :])
            pk[pl.ds(c * ext, low_rank, stride=2), :] = e0
            pk[pl.ds(c * ext + 1, low_rank, stride=2), :] = e1
        for c in range(low_rank):
            accw[t, :, c * 128:(c + 1) * 128] += pk[c * ext:c * ext + rank, :]
        for m in range(rank // 4):
            first = 2 * m
            turning[m] = jnp.transpose(stack(accw[t, :, first * 128:(first + 1) * 128], accw[t, :, (first + 1) * 128:(first + 2) * 128]))
        for m in range(rank // 8):
            lo, hi = turning[m], turning[m + rank // 8]
            l = lax.rem(lax.broadcasted_iota(jnp.int32, (ext, 128), 1), ext)
            for h in range(2):
                r = 4 * m + h
                x = jnp.where(l < rank, lo[h * ext:(h + 1) * ext], spread(hi[h * ext:(h + 1) * ext], m // 2))
                e0, e1 = halves(sv[pl.ds(r * pitch, half), :], sv[pl.ds((r + 2) * pitch, half), :])
                at = (2 * m + h) * ext
                pk[pl.ds(at, half, stride=2), :] = e0
                pk[pl.ds(at + 1, half, stride=2), :] = e1
                tile = slice((2 * m + h) * 128, (2 * m + h + 1) * 128)
                out[pl.ds(pl.multiple_of(t * ext, ext), ext), tile] = pk[at:at + ext, :] + x
        return 0

    lax.fori_loop(0, nb, finish, 0)


def contract(blocks, ownership, basis):
    slots, ext, area = blocks.shape
    size, rank = basis.shape
    nb = size // ext
    half = ext // 2
    u = basis.reshape(nb, ext, rank)
    ut = jnp.swapaxes(u, 1, 2)
    utp = u.reshape(nb, half, 2, rank).transpose(0, 3, 2, 1).reshape(nb, rank, ext)
    ub = jnp.pad(u, ((0, 0), (0, 0), (0, ext - rank)))
    count = jnp.sum((ownership[:, 0] >= 0).astype(jnp.int32)).reshape(1)
    sm = pl.BlockSpec(memory_space=pltpu.SMEM)
    vm = pl.BlockSpec(memory_space=pltpu.VMEM)
    return pl.pallas_call(
        functools.partial(contract_kernel, nb, ext, rank),
        out_shape=jax.ShapeDtypeStruct((size, rank // 2 * ext), f32),
        in_specs=[sm, sm, pl.BlockSpec(memory_space=pl.ANY), vm, vm, vm],
        out_specs=vm,
        scratch_shapes=[
            pltpu.VMEM((nb, rank, area), f32),
            pltpu.VMEM((nb, rank, rank * ext), f32),
            pltpu.VMEM((DEPTH, ext, area), bf16),
            pltpu.SemaphoreType.DMA((DEPTH,)),
            pltpu.VMEM((nb, 4 * ext, 4 * ext), bf16),
            pltpu.VMEM((3, ext, area), bf16),
            pltpu.VMEM((ext * (half + 1), 128), f32),
            pltpu.VMEM((rank * (half + 1), 128), f32),
            pltpu.VMEM((ext, area), bf16),
            pltpu.VMEM((rank // 2 * ext, 128), f32),
            pltpu.VMEM((half // 2, 128, 128), f32),
        ],
        compiler_params=pltpu.CompilerParams(vmem_limit_bytes=60 << 20),
    )(ownership.reshape(-1), count, blocks, ut, utp, ub)


def exchange_kernel(sizes, ext, part, y, out, near, ours, far, line, total, every, s_near, r_near, s_far, r_far, s_line, r_line, s_pair, r_pair, s_side, r_side, s_row, r_row):
    nx, nz, ng, rows, cols = sizes
    gx, gy, gz = lax.axis_index("gx"), lax.axis_index("gy"), lax.axis_index("gz")
    gh, core = gz // 2, lax.rem(gz, 2)
    side = [(a, b) for a in range(nx) for b in range(ng)]
    steps = side[1:] + side[:1]
    mate = (gx, gy, 2 * gh + 1 - core)

    def across(a, b):
        return lax.rem(gx + a, nx), lax.rem(gh + b, ng)

    def back(a, b):
        return lax.rem(gx + nx - a, nx), lax.rem(gh + ng - b, ng)

    def ahead(c):
        return lax.rem(gy + c, nz)

    def behind(c):
        return lax.rem(gy + nz - c, nz)

    def copy(src, dst, send, recv, device):
        return pltpu.make_async_remote_copy(
            src_ref=src, dst_ref=dst, send_sem=send, recv_sem=recv, device_id=device, device_id_type=MESH
        )

    def at_side(a, b):
        x, g = across(a, b)
        return (x, gy, 2 * g + core)

    def at_line(c):
        return (gx, ahead(c), gz)

    barrier = pltpu.get_barrier_semaphore()
    peers = [mate] + [at_side(a, b) for a, b in side[1:]] + [at_line(c) for c in range(1, nz)]
    for peer in peers:
        pl.semaphore_signal(barrier, inc=1, device_id=peer, device_id_type=MESH)
    pl.semaphore_wait(barrier, len(peers))

    pair = []
    for a, b in steps:
        x, g = across(a, b)
        m = a * ng + b
        c = copy(y.at[x, :, g, 1 - core], near.at[m], s_near.at[m], r_near.at[m], mate)
        c.start()
        pair.append(c)
    sent = []
    for (a, b), c in zip(steps, pair):
        x, g = across(a, b)
        m = a * ng + b
        c.wait_recv()
        for z in range(nz):
            ours[m, z] = (y[x, z, g, core] + near[m, z]).astype(bf16)
        if m:
            c = copy(ours.at[m], far.at[m], s_far.at[m], r_far.at[m], at_side(a, b))
            c.start()
            sent.append(c)
    for c in sent:
        c.wait_recv()
    hops = []
    for c in list(range(1, nz)) + [0]:
        z = ahead(c)
        t = ours[0, z].astype(f32)
        for m in range(1, len(side)):
            t = t + far[m, z].astype(f32)
        if c:
            line[c] = t.astype(bf16)
            d = copy(line.at[c], total.at[c], s_line.at[c], r_line.at[c], at_line(c))
            d.start()
            hops.append(d)
    for d in hops:
        d.wait_recv()
    for c in range(1, nz):
        t = t + total[c].astype(f32)
    mine = t.astype(bf16)

    def place(x, z, g, k):
        return ((x * nz + z) * ng + g) * 2 + k

    me = place(gx, gy, gh, core)
    every[me] = mine
    outgoing = []

    def send(where, sems, index, device):
        c = copy(every.at[where], every.at[where], sems[0].at[index], sems[1].at[index], device)
        c.start()
        outgoing.append(c)

    def landed(where, sems, index, device):
        copy(every.at[where], every.at[where], sems[0].at[index], sems[1].at[index], device).wait_recv()

    lines, sides, pairs = (s_row, r_row), (s_side, r_side), (s_pair, r_pair)
    for c in range(1, nz):
        send(me, lines, c, at_line(c))
    for m, (a, b) in enumerate(side[1:], 1):
        send(me, sides, m, at_side(a, b))
    send(me, pairs, 0, mate)
    for c in range(1, nz):
        where = place(gx, behind(c), gh, core)
        landed(where, lines, c, at_line(c))
        for m, (a, b) in enumerate(side[1:], 1):
            send(where, sides, c * len(side) + m, at_side(a, b))
        send(where, pairs, c * len(side), mate)
    for c in range(nz):
        for m, (a, b) in enumerate(side[1:], 1):
            x, g = back(a, b)
            where = place(x, behind(c), g, core)
            landed(where, sides, c * len(side) + m, at_side(a, b))
            send(where, pairs, c * len(side) + m, mate)
    for c in range(nz):
        for m, (a, b) in enumerate(side):
            x, g = back(a, b)
            landed(place(x, behind(c), g, 1 - core), pairs, c * len(side) + m, mate)
    for c in pair + sent + hops + outgoing:
        c.wait_send()

    l = lax.rem(lax.broadcasted_iota(jnp.int32, (rows, cols), 1), ext)
    once = (l < part) | ((l >= 2 * part) & (l < 2 * part + 8))
    weighted = (mine.astype(f32) * jnp.where(once, 1.0, 2.0)).astype(bf16)
    group = min(every.shape[0], 256 // rows)
    for first in range(0, every.shape[0], group):
        right = every[first:first + group].reshape(group * rows, cols)
        out[:, first * rows:(first + group) * rows] = lax.dot_general(
            weighted, right, (((1,), (1,)), ((), ())), preferred_element_type=f32
        )


def exchange(y, mesh_sizes, ext, part):
    x, z, g2 = mesh_sizes
    g = g2 // 2
    size, cols = y.shape
    devices = x * z * g2
    rows = size // devices
    m = x * g
    vm = pl.BlockSpec(memory_space=pltpu.VMEM)
    dma = lambda n: pltpu.SemaphoreType.DMA((n,))
    return pl.pallas_call(
        functools.partial(exchange_kernel, (x, z, g, rows, cols), ext, part),
        out_shape=jax.ShapeDtypeStruct((rows, size), f32),
        in_specs=[vm],
        out_specs=vm,
        scratch_shapes=[
            pltpu.VMEM((m, z, rows, cols), f32),
            pltpu.VMEM((m, z, rows, cols), bf16),
            pltpu.VMEM((m, z, rows, cols), bf16),
            pltpu.VMEM((z, rows, cols), bf16),
            pltpu.VMEM((z, rows, cols), bf16),
            pltpu.VMEM((devices, rows, cols), bf16),
            dma(m), dma(m), dma(m), dma(m), dma(z), dma(z),
            dma(z * m), dma(z * m), dma(z * m), dma(z * m), dma(z), dma(z),
        ],
        compiler_params=pltpu.CompilerParams(collective_id=0, has_side_effects=True, vmem_limit_bytes=48 << 20),
    )(y.reshape(x, z, g, 2, rows, cols))


def solution(mesh):
    sizes = tuple(mesh.shape[a] for a in AXES)

    def local(blocks, ownership, basis_rows):
        rank = basis_rows.shape[1]
        packed = contract(blocks, ownership, basis_rows)
        ext = blocks.shape[1]
        return exchange(packed, sizes, ext, rank // 2) / rank

    in_specs = (P(AXES, None, None), P(AXES, None), P())
    return jax.shard_map(local, mesh=mesh, in_specs=in_specs, out_specs=P(AXES, None), check_vma=False)
```

```python
import functools

import jax
import jax.numpy as jnp
from jax import lax
from jax.experimental import pallas as pl
from jax.experimental.pallas import tpu as pltpu
from jax.sharding import PartitionSpec as P

AXES = ("gx", "gy", "gz")
DEPTH = 3
f32, bf16 = jnp.float32, jnp.bfloat16
MESH = pl.DeviceIdType.MESH


def contract_kernel(nb, ext, rank, own, count, blocks, ut, utp, ub, out, accv, accw, buf, sems, bd, mask, sv, sw, vb, pk, turning, ready, gone):
    half = ext // 2
    pitch = half + 1
    width = 4 * ext
    chunks = ext * ext // width
    low_rank = rank // 2
    n = count[0]

    def fetch(s):
        return pltpu.make_async_copy(blocks.at[s], buf.at[lax.rem(s, DEPTH)], sems.at[lax.rem(s, DEPTH)])

    for s in range(DEPTH - 1):
        @pl.when(s < n)
        def _():
            fetch(s).start()

    lane = lax.broadcasted_iota(jnp.int32, (ext, width), 1)
    row = lax.broadcasted_iota(jnp.int32, (ext, width), 0)

    def prepare(b, _):
        u = ub[b]
        u4 = jnp.concatenate([u, u, u, u], axis=1)
        for y in range(4):
            bd[b, y * ext:(y + 1) * ext, :] = jnp.where(lane // ext == y, u4, 0)
        accv[b] = jnp.zeros(accv.shape[1:], f32)
        accw[b] = jnp.zeros(accw.shape[1:], f32)
        return 0

    lax.fori_loop(0, nb, prepare, 0)

    for c in range(chunks):
        y = lane // ext + 4 * c
        z = lax.rem(lane, ext)
        front = jnp.where(row < y, 1.0, jnp.where(row == y, 0.5, 0.0))
        back = jnp.where(y < z, 1.0, jnp.where(y == z, 0.5, 0.0))
        both = jnp.where((row == y) & (y == z), 1.0 / 6.0, front * back)
        cols = slice(c * width, (c + 1) * width)
        mask[0, :, cols] = front.astype(bf16)
        mask[1, :, cols] = back.astype(bf16)
        mask[2, :, cols] = both.astype(bf16)

    def halves(a, b):
        low = lax.broadcasted_iota(jnp.int32, a.shape, 1) < ext
        return jnp.where(low, a, pltpu.roll(b, ext, 1)), jnp.where(low, pltpu.roll(a, ext, 1), b)

    def gather(src, first):
        e0, e1 = halves(src[pl.ds(first * pitch, half), :], src[pl.ds((first + 1) * pitch, half), :])
        return jnp.concatenate([e0, e1], axis=0).astype(bf16)

    def step(s, _):
        cur = lax.rem(s, DEPTH)
        fetch(s).wait()

        @pl.when(s + DEPTH - 1 < n)
        def _():
            fetch(s + DEPTH - 1).start()

        i, j, k = own[3 * s], own[3 * s + 1], own[3 * s + 2]
        kind = jnp.where(j == k, jnp.where(i == j, 2, 1), 0)

        @pl.when((i == j) | (j == k))
        def _():
            for c in range(chunks):
                cols = slice(c * width, (c + 1) * width)
                buf[cur, :, cols] = buf[cur, :, cols] * mask[kind, :, cols]

        ui = ut[i]
        uj = utp[j]
        bdk = bd[k]
        for c in range(chunks):
            cols = slice(c * width, (c + 1) * width)
            t = buf[cur, :, cols]
            v = jnp.dot(t, bdk, preferred_element_type=f32)
            sv[pl.ds(2 * c, ext, stride=pitch), :] = v[:, :128]
            sv[pl.ds(2 * c + 1, ext, stride=pitch), :] = v[:, 128:]
            vb[:, cols] = v.astype(bf16)
            w = jnp.dot(ui, t, preferred_element_type=f32)
            sw[pl.ds(2 * c, rank, stride=pitch), :] = w[:, :128]
            sw[pl.ds(2 * c + 1, rank, stride=pitch), :] = w[:, 128:]
        for c in range(chunks):
            cols = slice(c * width, (c + 1) * width)
            accv[j, :, cols] += jnp.dot(ui, vb[:, cols], preferred_element_type=f32)
        for c in range(chunks):
            cols = slice(c * width, (c + 1) * width)
            e = jnp.concatenate([gather(sv, 4 * c), gather(sv, 4 * c + 2)], axis=1)
            accv[i, :, cols] += jnp.dot(uj, e, preferred_element_type=f32)
        for c in range(rank * ext // width):
            cols = slice(c * width, (c + 1) * width)
            e = jnp.concatenate([gather(sw, 4 * c), gather(sw, 4 * c + 2)], axis=1)
            accw[k, :, cols] += jnp.dot(uj, e, preferred_element_type=f32)
        return 0

    lax.fori_loop(0, n, step, 0)

    def spread(x, b):
        l = lax.rem(lax.broadcasted_iota(jnp.int32, x.shape, 1), ext)
        if b < 2:
            return pltpu.roll(x, low_rank - 8 * b, 1)
        return jnp.where(l < rank + 8, pltpu.roll(x, low_rank - 8 * b, 1), pltpu.roll(x, low_rank + 8, 1))

    def stack(a, b):
        pad = jnp.zeros((ext - rank, 128), f32)
        return jnp.concatenate([a, pad, b, pad], axis=0)

    def leave(t):
        slot = lax.rem(t, 2)
        return pltpu.make_async_copy(ready.at[slot], out.at[pl.ds(pl.multiple_of(t * ext, ext), ext), :], gone.at[slot])

    def finish(t, _):
        @pl.when(t >= 2)
        def _():
            leave(t - 2).wait()

        slot = lax.rem(t, 2)
        for g in range(half // 2):
            p0, p1 = accv[t, :, 256 * g:256 * g + 128], accv[t, :, 256 * g + 128:256 * g + 256]
            turning[g] = stack(*halves(p0, p1))
        for g in range(half // 2):
            turned = jnp.transpose(turning[g])
            for h in range(2):
                cols = slice((2 * g + h) * 128, (2 * g + h + 1) * 128)
                accv[t, :, cols] += turned[h * ext:h * ext + rank]
        for g in range(half):
            s = accv[t, :, g * 128:(g + 1) * 128]
            l = lax.rem(lax.broadcasted_iota(jnp.int32, (8, 128), 1), ext)
            for b in range(3):
                piece = jnp.where(l < rank, s[8 * b:8 * b + 8], spread(s[low_rank + 8 * b:low_rank + 8 * b + 8], b))
                sv[pl.ds(8 * b * pitch + g, 8, stride=pitch), :] = piece
        wpitch = low_rank + 1
        for c in range(low_rank):
            sw[pl.ds(c, rank, stride=wpitch), :] = accw[t, :, c * 128:(c + 1) * 128]
        for c in range(low_rank):
            e0, e1 = halves(sw[pl.ds(2 * c * wpitch, low_rank), :], sw[pl.ds((2 * c + 1) * wpitch, low_rank), :])
            pk[pl.ds(c * ext, low_rank, stride=2), :] = e0
            pk[pl.ds(c * ext + 1, low_rank, stride=2), :] = e1
        for c in range(low_rank):
            accw[t, :, c * 128:(c + 1) * 128] += pk[c * ext:c * ext + rank, :]
        for m in range(rank // 4):
            first = 2 * m
            turning[m] = jnp.transpose(stack(accw[t, :, first * 128:(first + 1) * 128], accw[t, :, (first + 1) * 128:(first + 2) * 128]))
        for m in range(rank // 8):
            lo, hi = turning[m], turning[m + rank // 8]
            l = lax.rem(lax.broadcasted_iota(jnp.int32, (ext, 128), 1), ext)
            for h in range(2):
                r = 4 * m + h
                x = jnp.where(l < rank, lo[h * ext:(h + 1) * ext], spread(hi[h * ext:(h + 1) * ext], m // 2))
                e0, e1 = halves(sv[pl.ds(r * pitch, half), :], sv[pl.ds((r + 2) * pitch, half), :])
                at = (2 * m + h) * ext
                pk[pl.ds(at, half, stride=2), :] = e0
                pk[pl.ds(at + 1, half, stride=2), :] = e1
                tile = slice((2 * m + h) * 128, (2 * m + h + 1) * 128)
                ready[slot, :, tile] = pk[at:at + ext, :] + x
        leave(t).start()
        return 0

    lax.fori_loop(0, nb, finish, 0)
    for t in range(max(nb - 2, 0), nb):
        leave(t).wait()


def contract(blocks, ownership, basis):
    slots, ext, area = blocks.shape
    size, rank = basis.shape
    nb = size // ext
    half = ext // 2
    u = basis.reshape(nb, ext, rank)
    ut = jnp.swapaxes(u, 1, 2)
    utp = u.reshape(nb, half, 2, rank).transpose(0, 3, 2, 1).reshape(nb, rank, ext)
    ub = jnp.pad(u, ((0, 0), (0, 0), (0, ext - rank)))
    count = jnp.sum((ownership[:, 0] >= 0).astype(jnp.int32)).reshape(1)
    sm = pl.BlockSpec(memory_space=pltpu.SMEM)
    vm = pl.BlockSpec(memory_space=pltpu.VMEM)
    return pl.pallas_call(
        functools.partial(contract_kernel, nb, ext, rank),
        out_shape=jax.ShapeDtypeStruct((size, rank // 2 * ext), f32),
        in_specs=[sm, sm, pl.BlockSpec(memory_space=pl.ANY), vm, vm, vm],
        out_specs=pl.BlockSpec(memory_space=pl.ANY),
        scratch_shapes=[
            pltpu.VMEM((nb, rank, area), f32),
            pltpu.VMEM((nb, rank, rank * ext), f32),
            pltpu.VMEM((DEPTH, ext, area), bf16),
            pltpu.SemaphoreType.DMA((DEPTH,)),
            pltpu.VMEM((nb, 4 * ext, 4 * ext), bf16),
            pltpu.VMEM((3, ext, area), bf16),
            pltpu.VMEM((ext * (half + 1), 128), f32),
            pltpu.VMEM((rank * (half + 1), 128), f32),
            pltpu.VMEM((ext, area), bf16),
            pltpu.VMEM((rank // 2 * ext, 128), f32),
            pltpu.VMEM((half // 2, 128, 128), f32),
            pltpu.VMEM((2, ext, rank // 2 * ext), f32),
            pltpu.SemaphoreType.DMA((2,)),
        ],
        compiler_params=pltpu.CompilerParams(vmem_limit_bytes=60 << 20),
    )(ownership.reshape(-1), count, blocks, ut, utp, ub)


def exchange_kernel(sizes, ext, part, y, out, kept, near, ours, far, line, total, every, s_kept, s_near, r_near, s_far, r_far, s_line, r_line, s_pair, r_pair, s_side, r_side, s_row, r_row):
    nx, nz, ng, rows, cols = sizes
    gx, gy, gz = lax.axis_index("gx"), lax.axis_index("gy"), lax.axis_index("gz")
    gh, core = gz // 2, lax.rem(gz, 2)
    side = [(a, b) for a in range(nx) for b in range(ng)]
    steps = side[1:] + side[:1]
    mate = (gx, gy, 2 * gh + 1 - core)

    def across(a, b):
        return lax.rem(gx + a, nx), lax.rem(gh + b, ng)

    def back(a, b):
        return lax.rem(gx + nx - a, nx), lax.rem(gh + ng - b, ng)

    def ahead(c):
        return lax.rem(gy + c, nz)

    def behind(c):
        return lax.rem(gy + nz - c, nz)

    def copy(src, dst, send, recv, device):
        return pltpu.make_async_remote_copy(
            src_ref=src, dst_ref=dst, send_sem=send, recv_sem=recv, device_id=device, device_id_type=MESH
        )

    def at_side(a, b):
        x, g = across(a, b)
        return (x, gy, 2 * g + core)

    def at_line(c):
        return (gx, ahead(c), gz)

    barrier = pltpu.get_barrier_semaphore()
    peers = [mate] + [at_side(a, b) for a, b in side[1:]] + [at_line(c) for c in range(1, nz)]
    for peer in peers:
        pl.semaphore_signal(barrier, inc=1, device_id=peer, device_id_type=MESH)
    pl.semaphore_wait(barrier, len(peers))

    order = list(range(1, nz)) + [0]
    wide = len(side)
    own, pair = {}, {}
    for c in order:
        pair[c] = copy(y.at[:, ahead(c), :, 1 - core], near.at[c], s_near.at[c], r_near.at[c], mate)
        pair[c].start()
        own[c] = pltpu.make_async_copy(y.at[:, ahead(c), :, core], kept.at[c], s_kept.at[c])
        own[c].start()
    sent = {}
    for c in order:
        own[c].wait()
        pair[c].wait_recv()
        for m, (a, b) in enumerate(steps, 1):
            m = m % wide
            x, g = across(a, b)
            ours[m, c] = (kept[c, x, g] + near[c, x, g]).astype(bf16)
            if m:
                sent[m, c] = copy(ours.at[m, c], far.at[m, c], s_far.at[m * nz + c], r_far.at[m * nz + c], at_side(a, b))
                sent[m, c].start()
    hops = {}
    for c in order:
        t = ours[0, c].astype(f32)
        for m in range(1, wide):
            sent[m, c].wait_recv()
            t = t + far[m, c].astype(f32)
        if c:
            line[c] = t.astype(bf16)
            hops[c] = copy(line.at[c], total.at[c], s_line.at[c], r_line.at[c], at_line(c))
            hops[c].start()
    for c in range(1, nz):
        hops[c].wait_recv()
        t = t + total[c].astype(f32)
    mine = t.astype(bf16)

    def place(x, z, g, k):
        return ((x * nz + z) * ng + g) * 2 + k

    me = place(gx, gy, gh, core)
    every[me] = mine
    outgoing = []

    def send(where, sems, index, device):
        c = copy(every.at[where], every.at[where], sems[0].at[index], sems[1].at[index], device)
        c.start()
        outgoing.append(c)

    def landed(where, sems, index):
        copy(every.at[where], every.at[where], sems[0].at[index], sems[1].at[index], mate).wait_recv()

    lines, sides, pairs = (s_row, r_row), (s_side, r_side), (s_pair, r_pair)
    straight = [(m, a, b) for m, (a, b) in enumerate(side) if (a == 0) != (b == 0)]
    corner = [(m, a, b) for m, (a, b) in enumerate(side) if a and b]

    def origin(c, a, b, k):
        x, g = back(a, b)
        return place(x, behind(c), g, k)

    def hand_out(c):
        where = origin(c, 0, 0, core)
        for m, a, b in straight:
            send(where, sides, c * wide + m, at_side(a, b))
        send(where, pairs, c * wide, mate)

    def relay(c):
        for m, a, b in straight:
            where = origin(c, a, b, core)
            landed(where, sides, c * wide + m)
            if a and c % 2 == 0:
                for o, (p, q) in enumerate(side):
                    if p == a and q:
                        send(where, sides, c * wide + o, at_side(0, q))
            if b and c % 2 == 1:
                for o, (p, q) in enumerate(side):
                    if q == b and p:
                        send(where, sides, c * wide + o, at_side(p, 0))
            send(where, pairs, c * wide + m, mate)

    for c in range(1, nz):
        send(me, lines, c, at_line(c))
    hand_out(0)
    for c in range(1, nz + 1):
        if c < nz:
            landed(origin(c, 0, 0, core), lines, c)
            hand_out(c)
        relay(c - 1)
    for c in range(nz):
        for m, a, b in corner:
            where = origin(c, a, b, core)
            landed(where, sides, c * wide + m)
            send(where, pairs, c * wide + m, mate)
    for c in range(nz):
        for m, (a, b) in enumerate(side):
            landed(origin(c, a, b, 1 - core), pairs, c * wide + m)
    for c in [*pair.values(), *sent.values(), *hops.values(), *outgoing]:
        c.wait_send()

    l = lax.rem(lax.broadcasted_iota(jnp.int32, (rows, cols), 1), ext)
    once = (l < part) | ((l >= 2 * part) & (l < 2 * part + 8))
    weighted = (mine.astype(f32) * jnp.where(once, 1.0, 2.0)).astype(bf16)
    group = min(every.shape[0], 256 // rows)
    for first in range(0, every.shape[0], group):
        right = every[first:first + group].reshape(group * rows, cols)
        out[:, first * rows:(first + group) * rows] = lax.dot_general(
            weighted, right, (((1,), (1,)), ((), ())), preferred_element_type=f32
        )


def exchange(y, mesh_sizes, ext, part):
    x, z, g2 = mesh_sizes
    g = g2 // 2
    size, cols = y.shape
    devices = x * z * g2
    rows = size // devices
    m = x * g
    vm = pl.BlockSpec(memory_space=pltpu.VMEM)
    dma = lambda n: pltpu.SemaphoreType.DMA((n,))
    return pl.pallas_call(
        functools.partial(exchange_kernel, (x, z, g, rows, cols), ext, part),
        out_shape=jax.ShapeDtypeStruct((rows, size), f32),
        in_specs=[pl.BlockSpec(memory_space=pl.ANY)],
        out_specs=vm,
        scratch_shapes=[
            pltpu.VMEM((z, x, g, rows, cols), f32),
            pltpu.VMEM((z, x, g, rows, cols), f32),
            pltpu.VMEM((m, z, rows, cols), bf16),
            pltpu.VMEM((m, z, rows, cols), bf16),
            pltpu.VMEM((z, rows, cols), bf16),
            pltpu.VMEM((z, rows, cols), bf16),
            pltpu.VMEM((devices, rows, cols), bf16),
            dma(z), dma(z), dma(z), dma(m * z), dma(m * z), dma(z), dma(z),
            dma(z * m), dma(z * m), dma(z * m), dma(z * m), dma(z), dma(z),
        ],
        compiler_params=pltpu.CompilerParams(collective_id=0, has_side_effects=True, vmem_limit_bytes=48 << 20),
    )(y.reshape(x, z, g, 2, rows, cols))


def solution(mesh):
    sizes = tuple(mesh.shape[a] for a in AXES)

    def local(blocks, ownership, basis_rows):
        rank = basis_rows.shape[1]
        packed = contract(blocks, ownership, basis_rows)
        ext = blocks.shape[1]
        return exchange(packed, sizes, ext, rank // 2) / rank

    in_specs = (P(AXES, None, None), P(AXES, None), P())
    return jax.shard_map(local, mesh=mesh, in_specs=in_specs, out_specs=P(AXES, None), check_vma=False)
```

```python
import functools

import jax
import jax.numpy as jnp
from jax import lax
from jax.experimental import pallas as pl
from jax.experimental.pallas import tpu as pltpu
from jax.sharding import PartitionSpec as P

AXES = ("gx", "gy", "gz")
DEPTH = 3
f32, bf16 = jnp.float32, jnp.bfloat16
MESH = pl.DeviceIdType.MESH


def contract_kernel(nb, ext, rank, own, blocks, ut, utp, ub, out, accv, accw, buf, sems, bd, mask, sv, sw, vb, pk, turning, turned2, ready, gone):
    half = ext // 2
    pitch = half + 1
    width = 4 * ext
    chunks = ext * ext // width
    low_rank = rank // 2
    n = lax.fori_loop(0, own.shape[0], lambda s, found: found + jnp.where(own[s, 0] >= 0, 1, 0), 0)

    def fetch(s):
        return pltpu.make_async_copy(blocks.at[s], buf.at[lax.rem(s, DEPTH)], sems.at[lax.rem(s, DEPTH)])

    for s in range(DEPTH - 1):
        @pl.when(s < n)
        def _():
            fetch(s).start()

    lane = lax.broadcasted_iota(jnp.int32, (ext, width), 1)
    row = lax.broadcasted_iota(jnp.int32, (ext, width), 0)

    def prepare(b, _):
        u = ub[b]
        u4 = jnp.concatenate([u, u, u, u], axis=1)
        for y in range(4):
            bd[b, y * ext:(y + 1) * ext, :] = jnp.where(lane // ext == y, u4, 0)
        accv[b] = jnp.zeros(accv.shape[1:], f32)
        accw[b] = jnp.zeros(accw.shape[1:], f32)
        return 0

    lax.fori_loop(0, nb, prepare, 0)

    for c in range(chunks):
        y = lane // ext + 4 * c
        z = lax.rem(lane, ext)
        front = jnp.where(row < y, 1.0, jnp.where(row == y, 0.5, 0.0))
        back = jnp.where(y < z, 1.0, jnp.where(y == z, 0.5, 0.0))
        both = jnp.where((row == y) & (y == z), 1.0 / 6.0, front * back)
        cols = slice(c * width, (c + 1) * width)
        mask[0, :, cols] = front.astype(bf16)
        mask[1, :, cols] = back.astype(bf16)
        mask[2, :, cols] = both.astype(bf16)

    def halves(a, b):
        low = lax.broadcasted_iota(jnp.int32, a.shape, 1) < ext
        return jnp.where(low, a, pltpu.roll(b, ext, 1)), jnp.where(low, pltpu.roll(a, ext, 1), b)

    def gather(src, first):
        e0, e1 = halves(src[pl.ds(first * pitch, half), :], src[pl.ds((first + 1) * pitch, half), :])
        return jnp.concatenate([e0, e1], axis=0).astype(bf16)

    def step(s, _):
        cur = lax.rem(s, DEPTH)
        fetch(s).wait()

        @pl.when(s + DEPTH - 1 < n)
        def _():
            fetch(s + DEPTH - 1).start()

        i, j, k = own[s, 0], own[s, 1], own[s, 2]
        kind = jnp.where(j == k, jnp.where(i == j, 2, 1), 0)

        @pl.when((i == j) | (j == k))
        def _():
            for c in range(chunks):
                cols = slice(c * width, (c + 1) * width)
                buf[cur, :, cols] = buf[cur, :, cols] * mask[kind, :, cols]

        ui = ut[i]
        uj = utp[j]
        bdk = bd[k]
        for first in range(0, chunks, 4):
            group = range(first, first + 4)
            t = {c: buf[cur, :, c * width:(c + 1) * width] for c in group}
            v4 = jnp.dot(jnp.concatenate([t[c] for c in group], axis=0), bdk, preferred_element_type=f32)
            for c in group:
                v = v4[(c - first) * ext:(c - first + 1) * ext]
                sv[pl.ds(2 * c, ext, stride=pitch), :] = v[:, :128]
                sv[pl.ds(2 * c + 1, ext, stride=pitch), :] = v[:, 128:]
                vb[:, c * width:(c + 1) * width] = v.astype(bf16)
            for c in group:
                w = jnp.dot(ui, t[c], preferred_element_type=f32)
                sw[pl.ds(2 * c, rank, stride=pitch), :] = w[:, :128]
                sw[pl.ds(2 * c + 1, rank, stride=pitch), :] = w[:, 128:]
        for c in range(chunks):
            cols = slice(c * width, (c + 1) * width)
            accv[j, :, cols] += jnp.dot(ui, vb[:, cols], preferred_element_type=f32)
        for c in range(chunks):
            cols = slice(c * width, (c + 1) * width)
            e = jnp.concatenate([gather(sv, 4 * c), gather(sv, 4 * c + 2)], axis=1)
            accv[i, :, cols] += jnp.dot(uj, e, preferred_element_type=f32)
        for c in range(rank * ext // width):
            cols = slice(c * width, (c + 1) * width)
            e = jnp.concatenate([gather(sw, 4 * c), gather(sw, 4 * c + 2)], axis=1)
            accw[k, :, cols] += jnp.dot(uj, e, preferred_element_type=f32)
        return 0

    lax.fori_loop(0, n, step, 0)

    def spread(x, b):
        l = lax.rem(lax.broadcasted_iota(jnp.int32, x.shape, 1), ext)
        if b < 2:
            return pltpu.roll(x, low_rank - 8 * b, 1)
        return jnp.where(l < rank + 8, pltpu.roll(x, low_rank - 8 * b, 1), pltpu.roll(x, low_rank + 8, 1))

    def stack(a, b):
        pad = jnp.zeros((ext - rank, 128), f32)
        return jnp.concatenate([a, pad, b, pad], axis=0)

    def leave(t):
        slot = lax.rem(t, 2)
        return pltpu.make_async_copy(ready.at[slot], out.at[pl.ds(pl.multiple_of(t * ext, ext), ext), :], gone.at[slot])

    def finish(t, _):
        @pl.when(t >= 2)
        def _():
            leave(t - 2).wait()

        slot = lax.rem(t, 2)
        wpitch = low_rank + 1
        for c in range(low_rank):
            sw[pl.ds(c, rank, stride=wpitch), :] = accw[t, :, c * 128:(c + 1) * 128]
        for c in range(low_rank):
            e0, e1 = halves(sw[pl.ds(2 * c * wpitch, low_rank), :], sw[pl.ds((2 * c + 1) * wpitch, low_rank), :])
            pk[pl.ds(c * ext, low_rank, stride=2), :] = e0
            pk[pl.ds(c * ext + 1, low_rank, stride=2), :] = e1
        for g in range(half // 2):
            p0, p1 = accv[t, :, 256 * g:256 * g + 128], accv[t, :, 256 * g + 128:256 * g + 256]
            turning[g] = stack(*halves(p0, p1))
        for c in range(low_rank):
            accw[t, :, c * 128:(c + 1) * 128] += pk[c * ext:c * ext + rank, :]
        for g in range(half // 2):
            turned = jnp.transpose(turning[g])
            for h in range(2):
                cols = slice((2 * g + h) * 128, (2 * g + h + 1) * 128)
                accv[t, :, cols] += turned[h * ext:h * ext + rank]
        for m in range(rank // 4):
            first = 2 * m
            turned2[m] = jnp.transpose(stack(accw[t, :, first * 128:(first + 1) * 128], accw[t, :, (first + 1) * 128:(first + 2) * 128]))
        for g in range(half):
            s = accv[t, :, g * 128:(g + 1) * 128]
            l = lax.rem(lax.broadcasted_iota(jnp.int32, (8, 128), 1), ext)
            for b in range(3):
                piece = jnp.where(l < rank, s[8 * b:8 * b + 8], spread(s[low_rank + 8 * b:low_rank + 8 * b + 8], b))
                sv[pl.ds(8 * b * pitch + g, 8, stride=pitch), :] = piece
        for m in range(rank // 8):
            lo, hi = turned2[m], turned2[m + rank // 8]
            l = lax.rem(lax.broadcasted_iota(jnp.int32, (ext, 128), 1), ext)
            for h in range(2):
                r = 4 * m + h
                x = jnp.where(l < rank, lo[h * ext:(h + 1) * ext], spread(hi[h * ext:(h + 1) * ext], m // 2))
                e0, e1 = halves(sv[pl.ds(r * pitch, half), :], sv[pl.ds((r + 2) * pitch, half), :])
                at = (2 * m + h) * ext
                pk[pl.ds(at, half, stride=2), :] = e0
                pk[pl.ds(at + 1, half, stride=2), :] = e1
                tile = slice((2 * m + h) * 128, (2 * m + h + 1) * 128)
                ready[slot, :, tile] = pk[at:at + ext, :] + x
        leave(t).start()
        return 0

    lax.fori_loop(0, nb, finish, 0)
    for t in range(max(nb - 2, 0), nb):
        leave(t).wait()


def contract(blocks, ownership, basis):
    slots, ext, area = blocks.shape
    size, rank = basis.shape
    nb = size // ext
    half = ext // 2
    u = basis.reshape(nb, ext, rank)
    ut = jnp.swapaxes(u, 1, 2)
    utp = u.reshape(nb, half, 2, rank).transpose(0, 3, 2, 1).reshape(nb, rank, ext)
    ub = jnp.pad(u, ((0, 0), (0, 0), (0, ext - rank)))
    sm = pl.BlockSpec(memory_space=pltpu.SMEM)
    vm = pl.BlockSpec(memory_space=pltpu.VMEM)
    return pl.pallas_call(
        functools.partial(contract_kernel, nb, ext, rank),
        out_shape=jax.ShapeDtypeStruct((size, rank // 2 * ext), f32),
        in_specs=[sm, pl.BlockSpec(memory_space=pl.ANY), vm, vm, vm],
        out_specs=pl.BlockSpec(memory_space=pl.ANY),
        scratch_shapes=[
            pltpu.VMEM((nb, rank, area), f32),
            pltpu.VMEM((nb, rank, rank * ext), f32),
            pltpu.VMEM((DEPTH, ext, area), bf16),
            pltpu.SemaphoreType.DMA((DEPTH,)),
            pltpu.VMEM((nb, 4 * ext, 4 * ext), bf16),
            pltpu.VMEM((3, ext, area), bf16),
            pltpu.VMEM((ext * (half + 1), 128), f32),
            pltpu.VMEM((rank * (half + 1), 128), f32),
            pltpu.VMEM((ext, area), bf16),
            pltpu.VMEM((rank // 2 * ext, 128), f32),
            pltpu.VMEM((half // 2, 128, 128), f32),
            pltpu.VMEM((rank // 4, 128, 128), f32),
            pltpu.VMEM((2, ext, rank // 2 * ext), f32),
            pltpu.SemaphoreType.DMA((2,)),
        ],
        compiler_params=pltpu.CompilerParams(vmem_limit_bytes=60 << 20),
    )(ownership, blocks, ut, utp, ub)


def exchange_kernel(sizes, ext, part, y, out, kept, near, ours, far, line, total, every, s_kept, s_near, r_near, s_far, r_far, s_line, r_line, s_pair, r_pair, s_side, r_side, s_row, r_row):
    nx, nz, ng, rows, cols = sizes
    gx, gy, gz = lax.axis_index("gx"), lax.axis_index("gy"), lax.axis_index("gz")
    gh, core = gz // 2, lax.rem(gz, 2)
    side = [(a, b) for a in range(nx) for b in range(ng)]
    steps = side[1:] + side[:1]
    mate = (gx, gy, 2 * gh + 1 - core)

    def across(a, b):
        return lax.rem(gx + a, nx), lax.rem(gh + b, ng)

    def back(a, b):
        return lax.rem(gx + nx - a, nx), lax.rem(gh + ng - b, ng)

    def ahead(c):
        return lax.rem(gy + c, nz)

    def behind(c):
        return lax.rem(gy + nz - c, nz)

    def copy(src, dst, send, recv, device):
        return pltpu.make_async_remote_copy(
            src_ref=src, dst_ref=dst, send_sem=send, recv_sem=recv, device_id=device, device_id_type=MESH
        )

    def at_side(a, b):
        x, g = across(a, b)
        return (x, gy, 2 * g + core)

    def at_line(c):
        return (gx, ahead(c), gz)

    barrier = pltpu.get_barrier_semaphore()
    peers = [mate] + [at_side(a, b) for a, b in side[1:]] + [at_line(c) for c in range(1, nz)]
    for peer in peers:
        pl.semaphore_signal(barrier, inc=1, device_id=peer, device_id_type=MESH)
    pl.semaphore_wait(barrier, len(peers))

    order = list(range(1, nz)) + [0]
    wide = len(side)
    own, pair = {}, {}
    for c in order:
        pair[c] = copy(y.at[:, ahead(c), :, 1 - core], near.at[c], s_near.at[c], r_near.at[c], mate)
        pair[c].start()
        own[c] = pltpu.make_async_copy(y.at[:, ahead(c), :, core], kept.at[c], s_kept.at[c])
        own[c].start()
    sent = {}
    for c in order:
        own[c].wait()
        pair[c].wait_recv()
        for m, (a, b) in enumerate(steps, 1):
            m = m % wide
            x, g = across(a, b)
            ours[m, c] = (kept[c, x, g] + near[c, x, g]).astype(bf16)
            if m:
                sent[m, c] = copy(ours.at[m, c], far.at[m, c], s_far.at[m * nz + c], r_far.at[m * nz + c], at_side(a, b))
                sent[m, c].start()
    hops = {}
    for c in order:
        t = ours[0, c].astype(f32)
        for m in range(1, wide):
            sent[m, c].wait_recv()
            t = t + far[m, c].astype(f32)
        if c:
            line[c] = t.astype(bf16)
            hops[c] = copy(line.at[c], total.at[c], s_line.at[c], r_line.at[c], at_line(c))
            hops[c].start()
    for c in range(1, nz):
        hops[c].wait_recv()
        t = t + total[c].astype(f32)
    mine = t.astype(bf16)

    def place(x, z, g, k):
        return ((x * nz + z) * ng + g) * 2 + k

    me = place(gx, gy, gh, core)
    every[me] = mine
    outgoing = []

    def send(where, sems, index, device):
        c = copy(every.at[where], every.at[where], sems[0].at[index], sems[1].at[index], device)
        c.start()
        outgoing.append(c)

    def landed(where, sems, index):
        copy(every.at[where], every.at[where], sems[0].at[index], sems[1].at[index], mate).wait_recv()

    lines, sides, pairs = (s_row, r_row), (s_side, r_side), (s_pair, r_pair)
    straight = [(m, a, b) for m, (a, b) in enumerate(side) if (a == 0) != (b == 0)]
    corner = [(m, a, b) for m, (a, b) in enumerate(side) if a and b]

    def origin(c, a, b, k):
        x, g = back(a, b)
        return place(x, behind(c), g, k)

    def hand_out(c):
        where = origin(c, 0, 0, core)
        for m, a, b in straight:
            send(where, sides, c * wide + m, at_side(a, b))
        send(where, pairs, c * wide, mate)

    def relay(c):
        for m, a, b in straight:
            where = origin(c, a, b, core)
            landed(where, sides, c * wide + m)
            if a and c % 2 == 0:
                for o, (p, q) in enumerate(side):
                    if p == a and q:
                        send(where, sides, c * wide + o, at_side(0, q))
            if b and c % 2 == 1:
                for o, (p, q) in enumerate(side):
                    if q == b and p:
                        send(where, sides, c * wide + o, at_side(p, 0))
            send(where, pairs, c * wide + m, mate)

    for c in range(1, nz):
        send(me, lines, c, at_line(c))
    hand_out(0)
    for c in range(1, nz + 1):
        if c < nz:
            landed(origin(c, 0, 0, core), lines, c)
            hand_out(c)
        relay(c - 1)
    for c in range(nz):
        for m, a, b in corner:
            where = origin(c, a, b, core)
            landed(where, sides, c * wide + m)
            send(where, pairs, c * wide + m, mate)
    for c in range(nz):
        for m, (a, b) in enumerate(side):
            landed(origin(c, a, b, 1 - core), pairs, c * wide + m)
    for c in [*pair.values(), *sent.values(), *hops.values(), *outgoing]:
        c.wait_send()

    l = lax.rem(lax.broadcasted_iota(jnp.int32, (rows, cols), 1), ext)
    once = (l < part) | ((l >= 2 * part) & (l < 2 * part + 8))
    weighted = (mine.astype(f32) * jnp.where(once, 1.0, 2.0)).astype(bf16)
    group = min(every.shape[0], 256 // rows)
    for first in range(0, every.shape[0], group):
        right = every[first:first + group].reshape(group * rows, cols)
        out[:, first * rows:(first + group) * rows] = lax.dot_general(
            weighted, right, (((1,), (1,)), ((), ())), preferred_element_type=f32
        )


def exchange(y, mesh_sizes, ext, part):
    x, z, g2 = mesh_sizes
    g = g2 // 2
    size, cols = y.shape
    devices = x * z * g2
    rows = size // devices
    m = x * g
    vm = pl.BlockSpec(memory_space=pltpu.VMEM)
    dma = lambda n: pltpu.SemaphoreType.DMA((n,))
    return pl.pallas_call(
        functools.partial(exchange_kernel, (x, z, g, rows, cols), ext, part),
        out_shape=jax.ShapeDtypeStruct((rows, size), f32),
        in_specs=[pl.BlockSpec(memory_space=pl.ANY)],
        out_specs=vm,
        scratch_shapes=[
            pltpu.VMEM((z, x, g, rows, cols), f32),
            pltpu.VMEM((z, x, g, rows, cols), f32),
            pltpu.VMEM((m, z, rows, cols), bf16),
            pltpu.VMEM((m, z, rows, cols), bf16),
            pltpu.VMEM((z, rows, cols), bf16),
            pltpu.VMEM((z, rows, cols), bf16),
            pltpu.VMEM((devices, rows, cols), bf16),
            dma(z), dma(z), dma(z), dma(m * z), dma(m * z), dma(z), dma(z),
            dma(z * m), dma(z * m), dma(z * m), dma(z * m), dma(z), dma(z),
        ],
        compiler_params=pltpu.CompilerParams(collective_id=0, has_side_effects=True, vmem_limit_bytes=48 << 20),
    )(y.reshape(x, z, g, 2, rows, cols))


def solution(mesh):
    sizes = tuple(mesh.shape[a] for a in AXES)

    def local(blocks, ownership, basis_rows):
        rank = basis_rows.shape[1]
        packed = contract(blocks, ownership, basis_rows)
        ext = blocks.shape[1]
        return exchange(packed, sizes, ext, rank // 2) / rank

    in_specs = (P(AXES, None, None), P(AXES, None), P())
    return jax.shard_map(local, mesh=mesh, in_specs=in_specs, out_specs=P(AXES, None), check_vma=False)
```
